256 devices in a mesh: seq: 128 (over z, y_hi, x, core), exp: 2 (over y_lo).
Axes of the slice: x: 4, y: 4 (y_hi: 2, y_lo: 2; y = y_hi * 2 + y_lo), z: 8, core: 2. Of those that a mesh axis runs over, the one named last changes fastest.
Arguments:
- queries: bfloat16 [49152, 1536], P('seq', 'exp'), may hold values from -120 to 120
- key_heads: bfloat16 [49152, 1536], P('seq', 'exp'), may hold values from -6 to 6
- value_heads: bfloat16 [49152, 1024], P('seq', 'exp'), may hold values from -6 to 6
- block_layout: int32 [384, 16], P('seq'), may hold values from 0 to 21, as said below
- out_weight: bfloat16 [1024, 2048], P('exp'), may hold values from -0.1875 to 0.1875
- norm_gain: float32 [2048], replicated, may hold values from 0.5 to 1.5
- expert_ids: int32 [49152, 1], P(('seq', 'exp')), may hold values from 0 to 1; in each aligned block of 192 rows (0 to 191, 192 to 383, ...) at most 144 rows name the same one
- route_weight: float32 [49152, 1], P(('seq', 'exp')), may hold values from 0.1 to 1
- gate_weight: bfloat16 [2, 2048, 704], P('exp'), may hold values from -0.125 to 0.125
- up_weight: bfloat16 [2, 2048, 704], P('exp'), may hold values from -0.125 to 0.125
- down_weight: bfloat16 [2, 704, 2048], P('exp'), may hold values from -0.21875 to 0.21875
Outputs:
- layer_out: bfloat16 [49152, 2048], P(('seq', 'exp'))
The draws below stay inside these ranges and needn't reach their ends.
Inputs may be any that keep to these rules, and one draw needn't show every extreme that they name: `block_layout`: each row holds the offset 0 and 15 other distinct offsets. `expert_ids`: among the 192 tokens of one device in the expert layer (aligned blocks of rows) at most 144 name the same expert.
All inputs are finite; a program needn't handle non-finite values.
Results may differ from the reference program's by a relative error of at most 0.02.
Values may be sent and summed in bfloat16 or wider, within the bound.
A program may use at most 128 MiB of HBM per device.

```python
import math
import jax
import jax.numpy as jnp
import numpy as np
from jax import lax

D = 2048
QK = 192
VD = 128
FF_E = 704
BLK = 128
TOK_DEV = 192
TOKENS = 49152
HEADS = 8
SPAN = 22
KSEL = 16
CAP = 144
N_EXP = 2


def pair_draw(key):
    base_key = jax.random.fold_in(key, 7)
    query_key, key_key = jax.random.split(base_key, 2)
    query_draw = jnp.clip(jax.random.normal(query_key, (TOKENS, HEADS * QK), jnp.float32), -6.0, 6.0)
    key_draw = jnp.clip(jax.random.normal(key_key, (TOKENS, HEADS * QK), jnp.float32), -6.0, 6.0)
    return (query_draw, key_draw)


def draw_queries(key, part):
    return pair_draw(key)[0].astype(jnp.bfloat16)


def draw_key_heads(key, part):
    return pair_draw(key)[1].astype(jnp.bfloat16)


def draw_block_layout(key, part):
    row_count = TOKENS // BLK
    random_bits = jax.random.randint(jax.random.fold_in(key, 11), (row_count, SPAN - 1), 0, 1 << 20) * SPAN + jnp.arange(SPAN - 1, dtype=jnp.int32)[None, :]
    ordering = jnp.argsort(random_bits, axis=1, stable=True)[:, :KSEL - 1].astype(jnp.int32) + 1
    return jnp.concatenate([jnp.zeros((row_count, 1), jnp.int32), ordering], axis=1)


def shard_levels(stream_key, dims, pieces, smallest, largest):
    def one(axis_at, blocks):
        steps = jax.random.uniform(jax.random.fold_in(jax.random.fold_in(stream_key, 6), axis_at), (blocks,), jnp.float32, smallest / len(pieces), largest / len(pieces))
        return jnp.repeat(jnp.exp(steps), dims[axis_at] // blocks).reshape((-1,) + (1,) * (len(dims) - axis_at - 1))

    loudness = one(*pieces[0])
    for cut in pieces[1:]:
        loudness = loudness * one(*cut)
    return loudness


def routed_block(stream_key, own, number, rows, count, top, reach, lean):
    order = jax.random.permutation(stream_key, count)
    heavy_load, usual = portions_of(count, rows * top, reach, lean, True), portions_of(count, rows * top, reach, lean, False)
    places = jnp.arange(count)

    def named(lengths, turn):
        used = int((lengths > 0).sum())
        fixed = max(1, used // 4)
        moved = fixed + (places - fixed + turn * (used - fixed)) % max(1, count - fixed)
        return jnp.zeros((count,), jnp.int32).at[order[jnp.where(places < fixed, places, moved)]].set(jnp.asarray(lengths, jnp.int32))

    lengths = jnp.where(number % 4 == 0, named(heavy_load, number // 4), named(usual, number - number // 4 - 1))
    mixed = jax.random.permutation(jax.random.fold_in(own, 3), count)
    source_of, receiver = mixed[0:count // 2 * 2:2], mixed[1:count // 2 * 2:2]
    margin = jnp.minimum(lengths[source_of] - 1, reach - lengths[receiver]) // 2
    margin = jnp.where((source_of == order[0]) | (receiver == order[0]) | (lengths[receiver] == 0), 0, jnp.maximum(margin, 0))
    moved = jax.random.randint(jax.random.fold_in(own, 4), (count // 2,), 0, 1 << 20) % (margin + 1)
    lengths = lengths.at[source_of].add(-moved).at[receiver].add(moved)
    items = jnp.searchsorted(jnp.cumsum(lengths), jnp.arange(rows * top), side="right").astype(jnp.int32)
    grid = items.reshape(top, rows).T
    grid = grid[jax.random.permutation(jax.random.fold_in(own, 1), rows)]
    turn = jax.random.randint(jax.random.fold_in(own, 2), (rows, 1), 0, top)
    return jnp.take_along_axis(grid, (jnp.arange(top)[None, :] + turn) % top, axis=1)


def portions_of(number_of, total, bound, skew, full):
    portions = [(1 << 20) // math.isqrt(grade ** skew) + 1 for grade in range(1, number_of + 1)]
    largest = bound if full else min(bound, max(-(-total // number_of), total * portions[0] // sum(portions)))
    least = 1 if total - largest >= number_of - 1 else 0
    counts, surplus = [largest] + [least] * (number_of - 1), total - largest - least * (number_of - 1)
    while surplus > 0:
        movable = [i for i in range(1, number_of) if counts[i] < largest] or [i for i in range(1, number_of) if counts[i] < bound]
        pool, left = sum([portions[i] for i in movable]), surplus
        for i in movable:
            extra = min(bound - counts[i], max(1, left * portions[i] // pool), surplus)
            counts[i] = counts[i] + extra
            surplus = surplus - extra
    return np.array(counts)


def centred(own_key, shape, deviation, most, pieces=(), held_as=jnp.bfloat16):
    entries = deviation * jax.random.normal(own_key, shape, jnp.float32)
    if pieces:
        entries = entries * shard_levels(own_key, shape, pieces, -0.22, 0.18)
    return jnp.clip(entries, -most, most).astype(held_as)


def setup_inputs(seed: int = 0) -> dict:
    keys = jax.random.split(jax.random.key(seed), 12)
    queries = draw_queries(jax.random.fold_in(keys[11], 71), 0)
    key_heads = draw_key_heads(jax.random.fold_in(keys[11], 71), 0)
    value_heads = centred(keys[2], (TOKENS, HEADS * VD), 1.0, 6.0, ((0, 128), (1, 2)))
    block_layout = draw_block_layout(jax.random.fold_in(keys[11], 71), 0)
    out_weight = centred(keys[4], (HEADS * VD, D), (HEADS * VD) ** -0.5, 0.1875, ((0, 2),))
    norm_gain = jnp.clip(1.0 + 0.1 * jax.random.normal(keys[5], (D,), jnp.float32), 0.5, 1.5)
    expert_ids_keys = jax.random.split(jax.random.fold_in(keys[6], 1), TOKENS // TOK_DEV)
    expert_ids_turns = jax.random.permutation(jax.random.fold_in(keys[6], 3), TOKENS // TOK_DEV)
    expert_ids = jax.vmap(lambda own, number: routed_block(jax.random.fold_in(keys[6], 2), own, number, TOK_DEV, N_EXP, 1, CAP, 1))(expert_ids_keys, expert_ids_turns).reshape((TOKENS, 1))
    route_weight = jnp.clip(jnp.exp(math.log(1.0) - 2.3025851 * jax.random.uniform(keys[7], (TOKENS, 1), jnp.float32) ** shard_levels(keys[7], (TOKENS, 1), ((0, 256),), -0.2, 0.2)), 0.1, 1.0)
    gate_weight = centred(keys[8], (N_EXP, D, FF_E), D ** -0.5, 0.125, ((0, 2),))
    up_weight = centred(keys[9], (N_EXP, D, FF_E), D ** -0.5, 0.125, ((0, 2),))
    down_weight = centred(keys[10], (N_EXP, FF_E, D), FF_E ** -0.5, 0.21875, ((0, 2),))
    return {"queries": queries, "key_heads": key_heads, "value_heads": value_heads, "block_layout": block_layout, "out_weight": out_weight, "norm_gain": norm_gain, "expert_ids": expert_ids, "route_weight": route_weight, "gate_weight": gate_weight, "up_weight": up_weight, "down_weight": down_weight}


def attend_block(block_index, queries, key_heads, value_heads, block_layout):
    within = jnp.arange(BLK, dtype=jnp.int32)
    first = block_index * BLK
    query_grid = lax.dynamic_slice_in_dim(queries, first, BLK, 0).astype(jnp.float32).reshape(BLK, HEADS, QK)
    anchor = block_index - block_layout[block_index]
    is_valid = anchor >= 0
    row_index = (jnp.maximum(anchor, 0)[:, None] * BLK + within[None, :]).reshape(-1)
    keys_sel = jnp.take(key_heads, row_index, axis=0).astype(jnp.float32).reshape(KSEL * BLK, HEADS, QK)
    values_sel = jnp.take(value_heads, row_index, axis=0).astype(jnp.float32).reshape(KSEL * BLK, HEADS, VD)
    scores = jnp.einsum('qhd,khd->hqk', query_grid, keys_sel) * QK ** (-0.5)
    key_pos = (anchor[:, None] * BLK + within[None, :]).reshape(-1)
    key_valid = jnp.repeat(is_valid, BLK)
    allowed = key_valid[None, :] & (key_pos[None, :] <= (first + within)[:, None])
    scores = jnp.where(allowed[None], scores, jnp.float32(-1e+30))
    row_peak = lax.optimization_barrier(jnp.max(scores, axis=2, keepdims=True))
    weights = jnp.exp(scores - row_peak)
    attn_probs = (weights / lax.optimization_barrier(jnp.sum(weights, axis=2, keepdims=True))).astype(jnp.bfloat16)
    attn_probs = lax.optimization_barrier(attn_probs).astype(jnp.float32)
    context = jnp.einsum('hqk,khd->qhd', attn_probs, values_sel)
    return context.astype(jnp.bfloat16).reshape(BLK, HEADS * VD)

def expert_apply(arrivals, gate_matrix, up_matrix, down_matrix):
    gate_part = jnp.dot(arrivals, gate_matrix, preferred_element_type=jnp.float32)
    up_part = jnp.dot(arrivals, up_matrix, preferred_element_type=jnp.float32)
    hidden = (jax.nn.silu(gate_part) * up_part).astype(jnp.bfloat16)
    return jnp.dot(hidden, down_matrix, preferred_element_type=jnp.float32).astype(jnp.bfloat16)

def reference(queries, key_heads, value_heads, block_layout, out_weight, norm_gain, expert_ids, route_weight, gate_weight, up_weight, down_weight):
    context = lax.map(lambda block_index: attend_block(block_index, queries, key_heads, value_heads, block_layout), jnp.arange(TOKENS // BLK, dtype=jnp.int32))
    context = context.reshape(TOKENS, HEADS * VD)
    attended = jnp.dot(context, out_weight, preferred_element_type=jnp.float32)
    rescale = lax.rsqrt(lax.optimization_barrier(jnp.mean(attended * attended, axis=1, keepdims=True)) + 1e-06)
    normed = (attended * rescale * norm_gain).astype(jnp.bfloat16)
    route_ids = expert_ids[:, 0]
    combined = jnp.zeros(attended.shape, jnp.float32)
    for expert in range(N_EXP):
        result = expert_apply(normed, gate_weight[expert], up_weight[expert], down_weight[expert]).astype(jnp.float32)
        combined = combined + jnp.where((route_ids == expert)[:, None], result, jnp.float32(0.0))
    return (attended + route_weight * combined).astype(jnp.bfloat16)
```

```python
import functools
import math

import jax
import jax.numpy as jnp
from jax import lax
from jax.experimental import pallas as pl
from jax.experimental.pallas import tpu as pltpu
from jax.sharding import PartitionSpec as P

MESH = pl.DeviceIdType.MESH
F32 = jnp.float32
BF16 = jnp.bfloat16
QK = 192
VD = 128
BLK = 128
TOK = 384
OWN = 192
SPAN = 22
CAP = 144
D = 2048
FF = 704
NCH = 4
WCH = D // NCH
KVR = 960
QR = 608
NEG = -1e30
COEF = QK ** (-0.5) * math.log2(math.e)


def half_turn(a):
    return pltpu.roll(a.astype(F32), 64, 1)


def low_lanes(shape):
    return lax.broadcasted_iota(jnp.int32, shape, 1) < 64


def pack_tail(tile, high):
    a = tile[:OWN].astype(F32)
    b = tile[OWN:].astype(F32)
    if high:
        a = pltpu.roll(a, 64, 1)
    else:
        b = pltpu.roll(b, 64, 1)
    return jnp.where(low_lanes(a.shape), a, b).astype(BF16)


def kernel(
    q_ref, k_ref, v_ref, lay_ref, gain_ref, ids_ref, rw_ref, ow_ref, gw_ref, uw_ref, dw_ref,
    out_ref,
    kst, qst, kv, kt, qraw, qb, bias, m_sc, l_sc, acc, cst, ctx, wb, gwb, uwb, dwb,
    idr, idm, att, nrm, rows, own_res, rst, ret, pm,
    ld, s_kv, r_kv, s_q, r_q, s_f, s_row, s_c, r_c, s_w, r_w, s_id, r_id, s_ret, r_ret,
):
    s = lax.axis_index("seq")
    e = lax.axis_index("exp")
    c = lax.rem(s, 2)
    x = lax.rem(s // 2, 4)
    r = s // 8
    p = lax.rem(s, 8)
    yh = lax.rem(r, 2)
    z = r // 2
    ct = x // 2

    def at(row, xx, cc, ee):
        return (row * 8 + xx * 2 + cc, ee)

    nxt = lax.rem(r + 1, 16)
    prv = lax.rem(r + 15, 16)
    cross = (z * 2 + (1 - yh)) * 8 + p
    up = (s + e * (cross - s), 1 - e)
    down = (cross + e * (s - cross), 1 - e)

    loads = [
        pltpu.make_async_copy(ow_ref, wb.at[e], ld.at[0]),
        pltpu.make_async_copy(gw_ref, gwb, ld.at[1]),
        pltpu.make_async_copy(uw_ref, uwb, ld.at[2]),
        pltpu.make_async_copy(dw_ref, dwb, ld.at[3]),
    ]
    for one in loads:
        one.start()

    bar = pltpu.get_barrier_semaphore()
    for dp in range(8):
        for de in range(2):
            if dp or de:
                who = (r * 8 + lax.rem(p + dp, 8), lax.rem(e + de, 2))
                pl.semaphore_signal(bar, inc=1, device_id=who, device_id_type=MESH)
    for row in (nxt, prv):
        for cc in range(2):
            pl.semaphore_signal(bar, inc=1, device_id=at(row, x, cc, e), device_id_type=MESH)
    pl.semaphore_signal(bar, inc=1, device_id=(cross, 1 - e), device_id_type=MESH)

    for h in range(4):
        main = (0, 2, 3, 5)[h]
        tail = (1, 1, 4, 4)[h]
        high = h % 2 == 1
        kst[h, 0:384] = k_ref[:, main * 128 : main * 128 + 128]
        kst[h, 384:576] = pack_tail(k_ref[:, tail * 128 : tail * 128 + 128], high)
        kst[h, 576:960] = v_ref[:, h * 128 : h * 128 + 128]
        qst[h, 0:384] = q_ref[:, main * 128 : main * 128 + 128]
        qst[h, 384:576] = pack_tail(q_ref[:, tail * 128 : tail * 128 + 128], high)
    row_i = lax.broadcasted_iota(jnp.int32, (32, 128), 0)
    lane_i = lax.broadcasted_iota(jnp.int32, (32, 128), 1)
    jq = lax.rem(row_i, 3)
    win = (row_i // 3) * 3 + lane_i
    off = SPAN - 1 + jq - win
    seen = jnp.zeros((32, 128), jnp.bool_)
    for t in range(16):
        mine = jnp.where(jq == 0, lay_ref[0, t], jnp.where(jq == 1, lay_ref[1, t], lay_ref[2, t]))
        seen = seen | (off == mine)
    seen = seen & (off >= 0) & (3 * s - (SPAN - 1) + win >= 0)
    mask = jnp.where(seen, 0.0, NEG).astype(BF16)
    for h in range(4):
        qst[h, 576:608] = mask
    col = jnp.broadcast_to(ids_ref[...].astype(F32), (OWN, 128))
    col = jnp.concatenate([col, jnp.full((64, 128), 5.0, F32)], axis=0)
    idm[...] = jnp.transpose(col)[0:8]

    pl.semaphore_wait(bar, 20)

    w_out = []
    for d, who in ((0, up), (1, down)):
        quarter = pl.multiple_of((2 * c + d) * 128, 128)
        one = pltpu.make_async_remote_copy(
            src_ref=ow_ref.at[pl.ds(quarter, 128)],
            dst_ref=wb.at[e, pl.ds(quarter, 128)],
            send_sem=s_w.at[d],
            recv_sem=r_w.at[2 * c + d],
            device_id=who,
            device_id_type=MESH,
        )
        one.start()
        w_out.append(one)
    send_id = pltpu.make_async_remote_copy(
        src_ref=idm, dst_ref=idr, send_sem=s_id, recv_sem=r_id, device_id=(s, 1 - e), device_id_type=MESH
    )
    send_id.start()

    def kv_copy(d):
        xx = lax.rem(x + d, 4)
        return pltpu.make_async_remote_copy(
            src_ref=kst.at[xx], dst_ref=kv.at[8 + p], send_sem=s_kv.at[d], recv_sem=r_kv.at[8 + p],
            device_id=at(r, xx, ct, e), device_id_type=MESH,
        )

    def q_copy(d):
        xx = lax.rem(x + d, 4)
        return pltpu.make_async_remote_copy(
            src_ref=qst.at[xx], dst_ref=qraw.at[lax.rem(p, 4)], send_sem=s_q.at[d], recv_sem=r_q.at[lax.rem(p, 4)],
            device_id=at(r, xx, ct, e), device_id_type=MESH,
        )

    for copy_of in (kv_copy, q_copy):
        for d in (1, 3, 2):
            copy_of(d).start()

        @pl.when(c != ct)
        def _():
            copy_of(0).start()

    @pl.when(c == ct)
    def _():
        kv[8 + p] = kst[x]
        qraw[lax.rem(p, 4)] = qst[x]

    def kv_wait(slot):
        pltpu.make_async_remote_copy(
            src_ref=kst.at[0], dst_ref=kv.at[slot], send_sem=s_kv.at[0], recv_sem=r_kv.at[slot],
            device_id=at(r, x, 1 - c, e), device_id_type=MESH,
        ).wait_recv()

    def to_core1(slot):
        return pltpu.make_async_remote_copy(
            src_ref=kv.at[slot], dst_ref=kv.at[slot], send_sem=s_f.at[slot], recv_sem=r_kv.at[slot],
            device_id=at(r, x, 1, e), device_id_type=MESH,
        )

    def to_next(slot):
        return pltpu.make_async_remote_copy(
            src_ref=kv.at[slot], dst_ref=kv.at[slot - 8], send_sem=s_row.at[slot - 8], recv_sem=r_kv.at[slot - 8],
            device_id=at(nxt, x, 0, e), device_id_type=MESH,
        )

    def unpack(slot):
        t = kv[slot, 384:576]
        kt[slot, 0:192] = t
        kt[slot, 192:384] = half_turn(t).astype(BF16)

    def clear(g, carry):
        m_sc[g] = jnp.full((TOK, 128), -3e38, F32)
        l_sc[g] = jnp.zeros((TOK, 128), F32)
        acc[g] = jnp.zeros((TOK, 128), F32)
        return carry

    lax.fori_loop(0, 4, clear, 0)

    def arrive(i, carry):
        slot = 8 + 4 * c + lax.rem(2 * lax.rem(x, 2) + 2 * (1 - lax.rem(x, 2)) * 0 + i, 4)

        @pl.when(slot != 8 + p)
        def _():
            kv_wait(slot)

        @pl.when(slot > 8)
        def _():
            to_next(slot).start()

        @pl.when(c == 0)
        def _():
            to_core1(slot).start()

        unpack(slot)
        return carry

    lax.fori_loop(0, 4, arrive, 0)

    def take_q(g, carry):
        @pl.when(4 * c + g != p)
        def _():
            pltpu.make_async_remote_copy(
                src_ref=qst.at[0], dst_ref=qraw.at[g], send_sem=s_q.at[0], recv_sem=r_q.at[g],
                device_id=at(r, x, 1 - c, e), device_id_type=MESH,
            ).wait_recv()

        qb[g, :, 0:128] = qraw[g, 0:384]
        t = qraw[g, 384:576].astype(F32)
        low = low_lanes(t.shape)
        qb[g, 0:192, 128:256] = jnp.where(low, t, 0.0).astype(BF16)
        qb[g, 192:384, 128:256] = jnp.where(low, half_turn(t), 0.0).astype(BF16)
        b = qraw[g, 576:608].astype(F32)
        for j in range(3):
            bias[g, :, j * 128 : j * 128 + 128] = jnp.broadcast_to(b[:, j : j + 1], (32, 128))
        return carry

    lax.fori_loop(0, 4, take_q, 0)

    def tile(g, slot, diag):
        keys = jnp.concatenate([kv[slot, 0:384], kt[slot]], axis=1)
        vals = kv[slot, 576:960]
        sc = lax.dot_general(qb[g], keys, (((1,), (1,)), ((), ())), preferred_element_type=F32)
        k = slot - (4 * c + g) - 1
        for j in range(3):
            own = slice(j * 128, j * 128 + 128)
            sj = sc[own] + bias[g, pl.ds(3 * k + j, 1), :]
            if diag:
                qi = lax.broadcasted_iota(jnp.int32, (128, TOK), 0) + j * 128
                ki = lax.broadcasted_iota(jnp.int32, (128, TOK), 1)
                sj = jnp.where(ki <= qi, sj, NEG)
            top = jnp.maximum(jnp.maximum(sj[:, 0:128], sj[:, 128:256]), sj[:, 256:384])
            m_old = m_sc[g, own]
            m_new = jnp.maximum(m_old, jnp.max(top, axis=1, keepdims=True))
            fade = jnp.exp2((m_old - m_new) * COEF)
            parts = [jnp.exp2((sj[:, i * 128 : i * 128 + 128] - m_new) * COEF) for i in range(3)]
            m_sc[g, own] = m_new
            l_sc[g, own] = l_sc[g, own] * fade + (parts[0] + parts[1] + parts[2])
            pr = jnp.concatenate([a.astype(BF16) for a in parts], axis=1)
            acc[g, own] = acc[g, own] * fade + jnp.dot(pr, vals, preferred_element_type=F32)

    def own_row(i, carry):
        slot = 8 + i

        @pl.when((c == 1) & (i < 4))
        def _():
            kv_wait(slot)
            unpack(slot)

        first = i - 4 * c

        @pl.when(first >= 0)
        def _():
            tile(first, slot, True)

        def inner(g, carry2):
            tile(g, slot, False)
            return carry2

        lax.fori_loop(jnp.maximum(first + 1, 0), 4, inner, 0)
        return carry

    lax.fori_loop(0, 4 + 4 * c, own_row, 0)

    def prev_row(i, carry):
        half = i // 2
        odd = i - 2 * half
        slot = (1 - c) * (7 - 4 * odd - half) + c * (7 - i)
        kv_wait(slot)

        @pl.when((c == 0) & (slot >= 5))
        def _():
            to_core1(slot).start()

        unpack(slot)

        def inner(g, carry2):
            tile(g, slot, False)
            return carry2

        lax.fori_loop(0, jnp.minimum(slot - 4 * c, 4), inner, 0)
        return carry

    lax.fori_loop(0, 7 - 4 * c, prev_row, 0)

    head = 4 * e + x

    def ctx_copy(g, de):
        return pltpu.make_async_remote_copy(
            src_ref=cst.at[g], dst_ref=ctx.at[head], send_sem=s_c.at[2 * g + de], recv_sem=r_c.at[head],
            device_id=at(r, 2 * c + g // 2, lax.rem(g, 2), lax.rem(e + de, 2)), device_id_type=MESH,
        )

    def finish(g, carry):
        total = jnp.sum(l_sc[g], axis=1, keepdims=True)
        cst[g] = (acc[g] / total).astype(BF16)
        ctx_copy(g, 1).start()

        @pl.when(4 * c + g != p)
        def _():
            ctx_copy(g, 0).start()

        @pl.when(4 * c + g == p)
        def _():
            ctx[head] = cst[g]

        return carry

    lax.fori_loop(0, 4, finish, 0)

    def w_copy(quarter):
        start = pl.multiple_of(quarter * 128, 128)
        return pltpu.make_async_remote_copy(
            src_ref=wb.at[1 - e, pl.ds(start, 128)], dst_ref=wb.at[1 - e, pl.ds(start, 128)],
            send_sem=s_w.at[2 + lax.rem(quarter, 2)], recv_sem=r_w.at[quarter],
            device_id=at(r, x, 1 - c, e), device_id_type=MESH,
        )

    for d in range(2):
        w_copy(2 * c + d).wait_recv()
        w_copy(2 * c + d).start()

    send_id.wait_recv()
    upper = (
        lax.broadcasted_iota(jnp.int32, (256, 256), 0) <= lax.broadcasted_iota(jnp.int32, (256, 256), 1)
    ).astype(BF16)
    for n, (src, who) in enumerate(((idr, e), (idm, e), (idm, 1 - e))):
        member = (src[...] == who.astype(F32)).astype(F32)
        member = jnp.concatenate([member, member], axis=0)
        rank = jnp.dot(member.astype(BF16), upper, preferred_element_type=F32)
        rank = jnp.where(member > 0.5, rank - 1.0, -1.0)[0:1]
        slots = lax.broadcasted_iota(jnp.int32, (CAP, 256), 0).astype(F32)
        pm[n] = jnp.where(slots == rank, 1.0, 0.0).astype(BF16)

    for one in loads:
        one.wait()
    for d in range(2):
        w_copy(2 * (1 - c) + d).wait_recv()

    def ctx_wait(h, carry):
        @pl.when((h != head) | (c != ct))
        def _():
            pltpu.make_async_remote_copy(
                src_ref=cst.at[0], dst_ref=ctx.at[h], send_sem=s_c.at[0], recv_sem=r_c.at[h],
                device_id=at(r, x, 1 - c, e), device_id_type=MESH,
            ).wait_recv()

        return carry

    lax.fori_loop(0, 8, ctx_wait, 0)

    def project(n, carry):
        cols = pl.ds(pl.multiple_of(n * WCH, WCH), WCH)
        total = jnp.zeros((TOK, WCH), F32)
        for side in range(2):
            left = jnp.concatenate([ctx[4 * side + i] for i in range(4)], axis=1)
            total = total + jnp.dot(left, wb[side, :, cols], preferred_element_type=F32)
        att[:, cols] = total
        sq = total * total
        part = sq[:, 0:128]
        for i in range(1, WCH // 128):
            part = part + sq[:, i * 128 : i * 128 + 128]
        return carry + part

    sums = lax.fori_loop(0, NCH, project, jnp.zeros((TOK, 128), F32))
    scale = lax.rsqrt(jnp.sum(sums, axis=1, keepdims=True) * (1.0 / D) + 1e-06)

    def normalize(n, carry):
        cols = pl.ds(pl.multiple_of(n * WCH, WCH), WCH)
        val = (att[:, cols] * scale * gain_ref[:, cols]).astype(BF16)
        for side in range(2):
            nrm[side, 0:OWN, cols] = val[side * OWN : side * OWN + OWN]
            nrm[side, OWN:256, cols] = jnp.zeros((64, WCH), BF16)
        rows[0:CAP, cols] = jnp.dot(pm[0], nrm[1 - e, :, cols], preferred_element_type=F32).astype(BF16)
        rows[CAP : 2 * CAP, cols] = jnp.dot(pm[1], nrm[e, :, cols], preferred_element_type=F32).astype(BF16)
        return carry

    lax.fori_loop(0, NCH, normalize, 0)

    gate = jnp.dot(rows[...], gwb[...], preferred_element_type=F32)
    upp = jnp.dot(rows[...], uwb[...], preferred_element_type=F32)
    hidden = (gate * jax.nn.sigmoid(gate) * upp).astype(BF16)

    def ret_copy(n):
        return pltpu.make_async_remote_copy(
            src_ref=rst.at[n], dst_ref=ret.at[n], send_sem=s_ret.at[n], recv_sem=r_ret.at[n],
            device_id=(s, 1 - e), device_id_type=MESH,
        )

    for n in range(NCH):
        cols = slice(n * WCH, n * WCH + WCH)
        res = jnp.dot(hidden, dwb[:, cols], preferred_element_type=F32).astype(BF16)
        rst[n] = res[0:CAP]
        own_res[n] = res[CAP : 2 * CAP]
        ret_copy(n).start()

    for n in range(NCH):
        cols = slice(n * WCH, n * WCH + WCH)
        got = lax.dot_general(pm[1], own_res[n], (((0,), (0,)), ((), ())), preferred_element_type=F32)
        ret_copy(n).wait_recv()
        got = got + lax.dot_general(pm[2], ret[n], (((0,), (0,)), ((), ())), preferred_element_type=F32)
        base = att[pl.ds(pl.multiple_of(e * OWN, OWN), OWN), cols]
        out_ref[:, cols] = (base + rw_ref[...] * got[0:OWN]).astype(BF16)

    for n in range(NCH):
        ret_copy(n).wait_send()
    for d in (1, 2, 3):
        kv_copy(d).wait_send()
        q_copy(d).wait_send()

    @pl.when(c != ct)
    def _():
        kv_copy(0).wait_send()
        q_copy(0).wait_send()

    def sent(i, carry):
        slot = 8 + 4 * c + i

        @pl.when(slot > 8)
        def _():
            to_next(slot).wait_send()

        @pl.when(c == 0)
        def _():
            to_core1(slot).wait_send()

        return carry

    lax.fori_loop(0, 4, sent, 0)

    def sent_prev(i, carry):
        to_core1(5 + i).wait_send()
        return carry

    lax.fori_loop(0, 3 - 3 * c, sent_prev, 0)

    def sent_ctx(g, carry):
        ctx_copy(g, 1).wait_send()

        @pl.when(4 * c + g != p)
        def _():
            ctx_copy(g, 0).wait_send()

        return carry

    lax.fori_loop(0, 4, sent_ctx, 0)
    for one in w_out:
        one.wait_send()
    for d in range(2):
        w_copy(2 * c + d).wait_send()
    send_id.wait_send()


def shards(
    queries, key_heads, value_heads, block_layout, out_weight, norm_gain, expert_ids, route_weight,
    gate_weight, up_weight, down_weight,
):
    vm = pl.BlockSpec(memory_space=pltpu.VMEM)
    anyspace = pl.BlockSpec(memory_space=pl.ANY)
    dma = pltpu.SemaphoreType.DMA
    return pl.pallas_call(
        kernel,
        out_shape=jax.ShapeDtypeStruct((OWN, D), BF16),
        in_specs=[vm, vm, vm, pl.BlockSpec(memory_space=pltpu.SMEM), vm, vm, vm] + [anyspace] * 4,
        out_specs=vm,
        scratch_shapes=[
            pltpu.VMEM((4, KVR, 128), BF16),
            pltpu.VMEM((4, QR, 128), BF16),
            pltpu.VMEM((16, KVR, 128), BF16),
            pltpu.VMEM((16, TOK, 128), BF16),
            pltpu.VMEM((4, QR, 128), BF16),
            pltpu.VMEM((4, TOK, 256), BF16),
            pltpu.VMEM((4, 32, TOK), F32),
            pltpu.VMEM((4, TOK, 128), F32),
            pltpu.VMEM((4, TOK, 128), F32),
            pltpu.VMEM((4, TOK, 128), F32),
            pltpu.VMEM((4, TOK, 128), BF16),
            pltpu.VMEM((8, TOK, 128), BF16),
            pltpu.VMEM((2, 512, D), BF16),
            pltpu.VMEM((D, FF), BF16),
            pltpu.VMEM((D, FF), BF16),
            pltpu.VMEM((FF, D), BF16),
            pltpu.VMEM((8, 256), F32),
            pltpu.VMEM((8, 256), F32),
            pltpu.VMEM((TOK, D), F32),
            pltpu.VMEM((2, 256, D), BF16),
            pltpu.VMEM((2 * CAP, D), BF16),
            pltpu.VMEM((NCH, CAP, WCH), BF16),
            pltpu.VMEM((NCH, CAP, WCH), BF16),
            pltpu.VMEM((NCH, CAP, WCH), BF16),
            pltpu.VMEM((3, CAP, 256), BF16),
            dma((4,)),
            dma((4,)), dma((16,)),
            dma((4,)), dma((4,)),
            dma((16,)), dma((8,)),
            dma((8,)), dma((8,)),
            dma((4,)), dma((4,)),
            dma, dma,
            dma((NCH,)), dma((NCH,)),
        ],
        compiler_params=pltpu.CompilerParams(
            collective_id=0, has_side_effects=True, vmem_limit_bytes=60 * 1024 * 1024
        ),
        name="layer",
    )(
        queries, key_heads, value_heads, block_layout, norm_gain.reshape(1, D), expert_ids, route_weight,
        out_weight, gate_weight[0], up_weight[0], down_weight[0],
    )


def solution(mesh):
    in_specs = (
        P("seq", "exp"),
        P("seq", "exp"),
        P("seq", "exp"),
        P("seq", None),
        P("exp", None),
        P(),
        P(("seq", "exp"), None),
        P(("seq", "exp"), None),
        P("exp", None, None),
        P("exp", None, None),
        P("exp", None, None),
    )
    out_specs = P(("seq", "exp"), None)
    return jax.shard_map(shards, mesh=mesh, in_specs=in_specs, out_specs=out_specs, check_vma=False)
```

```python
import functools
import math

import jax
import jax.numpy as jnp
from jax import lax
from jax.experimental import pallas as pl
from jax.experimental.pallas import tpu as pltpu
from jax.sharding import PartitionSpec as P

MESH = pl.DeviceIdType.MESH
F32 = jnp.float32
BF16 = jnp.bfloat16
QK = 192
VD = 128
BLK = 128
TOK = 384
OWN = 192
SPAN = 22
CAP = 144
D = 2048
FF = 704
NCH = 4
WCH = D // NCH
PAIR = 768
KVR = 960
QR = 736
NEG = -1e30
COEF = QK ** (-0.5) * math.log2(math.e)


def half_turn(a):
    return pltpu.roll(a.astype(F32), 64, 1)


def turned(a):
    return jnp.transpose(a.astype(F32)).astype(BF16)


def low_lanes(shape):
    return lax.broadcasted_iota(jnp.int32, shape, 1) < 64


def pack_tail(tile, high):
    a = tile[:OWN].astype(F32)
    b = tile[OWN:].astype(F32)
    if high:
        a = pltpu.roll(a, 64, 1)
    else:
        b = pltpu.roll(b, 64, 1)
    return jnp.where(low_lanes(a.shape), a, b).astype(BF16)


def kernel(
    q_hbm, k_hbm, v_hbm, lay_ref, gain_ref, ids_ref, rw_ref, ow_ref, gw_ref, uw_ref, dw_ref,
    out_ref,
    q_ref, k_ref, v_ref, kst, qst, kv, kt, qraw, qb, bias, m_sc, l_sc, acc, sa, sb, pa, pb, cst, ctx, wb, gwb, uwb, dwb,
    idr, idm, rwr, rwc, att, nrm, rows, own_res, rst, ret, pm,
    ld, s_kv, r_kv, s_q, r_q, s_f, s_row, s_c, r_c, s_w, r_w, s_id, r_id, s_ret, r_ret,
):
    s = lax.axis_index("seq")
    e = lax.axis_index("exp")
    c = lax.rem(s, 2)
    x = lax.rem(s // 2, 4)
    r = s // 8
    p = lax.rem(s, 8)
    yh = lax.rem(r, 2)
    z = r // 2
    ct = x // 2

    def at(row, xx, cc, ee):
        return (row * 8 + xx * 2 + cc, ee)

    nxt = lax.rem(r + 1, 16)
    prv = lax.rem(r + 15, 16)
    cross = (z * 2 + (1 - yh)) * 8 + p
    up = (s + e * (cross - s), 1 - e)
    down = (cross + e * (s - cross), 1 - e)

    bar = pltpu.get_barrier_semaphore()
    for dp in range(8):
        for de in range(2):
            if dp or de:
                who = (r * 8 + lax.rem(p + dp, 8), lax.rem(e + de, 2))
                pl.semaphore_signal(bar, inc=1, device_id=who, device_id_type=MESH)
    for row in (nxt, prv):
        for cc in range(2):
            pl.semaphore_signal(bar, inc=1, device_id=at(row, x, cc, e), device_id_type=MESH)
    pl.semaphore_signal(bar, inc=1, device_id=(cross, 1 - e), device_id_type=MESH)

    load_k = pltpu.make_async_copy(k_hbm, k_ref, ld.at[4])
    load_v = pltpu.make_async_copy(v_hbm, v_ref, ld.at[5])
    load_q = pltpu.make_async_copy(q_hbm, q_ref, ld.at[6])
    loads = [
        pltpu.make_async_copy(ow_ref, wb.at[e], ld.at[0]),
        pltpu.make_async_copy(gw_ref, gwb, ld.at[1]),
        pltpu.make_async_copy(uw_ref, uwb, ld.at[2]),
        pltpu.make_async_copy(dw_ref, dwb, ld.at[3]),
    ]
    for one in [load_k, load_v, load_q] + loads:
        one.start()

    load_k.wait()
    load_v.wait()
    for h in range(4):
        main = (0, 2, 3, 5)[h]
        tail = (1, 1, 4, 4)[h]
        kst[h, 0:384] = k_ref[:, main * 128 : main * 128 + 128]
        kst[h, 384:576] = pack_tail(k_ref[:, tail * 128 : tail * 128 + 128], h % 2 == 1)
        for j in range(3):
            kst[h, 576 + j * 128 : 704 + j * 128] = turned(v_ref[j * 128 : j * 128 + 128, h * 128 : h * 128 + 128])

    pl.semaphore_wait(bar, 20)

    def kv_copy(d):
        xx = lax.rem(x + d, 4)
        return pltpu.make_async_remote_copy(
            src_ref=kst.at[xx], dst_ref=kv.at[8 + p], send_sem=s_kv.at[d], recv_sem=r_kv.at[8 + p],
            device_id=at(r, xx, ct, e), device_id_type=MESH,
        )

    def q_copy(d):
        xx = lax.rem(x + d, 4)
        return pltpu.make_async_remote_copy(
            src_ref=qst.at[xx], dst_ref=qraw.at[lax.rem(p, 4)], send_sem=s_q.at[d], recv_sem=r_q.at[lax.rem(p, 4)],
            device_id=at(r, xx, ct, e), device_id_type=MESH,
        )

    def spread(copy_of):
        for d in (1, 3, 2):
            copy_of(d).start()

        @pl.when(c != ct)
        def _():
            copy_of(0).start()

    spread(kv_copy)

    load_q.wait()
    for j in range(3):
        for t in range(6):
            piece = turned(q_ref[j * 128 : j * 128 + 128, t * 128 : t * 128 + 128])
            if t in (0, 2, 3, 5):
                h = {0: 0, 2: 1, 3: 2, 5: 3}[t]
                qst[h, j * 192 : j * 192 + 128] = piece
            else:
                h = {1: 0, 4: 2}[t]
                qst[h, j * 192 + 128 : j * 192 + 192] = piece[0:64]
                qst[h + 1, j * 192 + 128 : j * 192 + 192] = piece[64:128]
    row_i = lax.broadcasted_iota(jnp.int32, (160, 128), 0)
    jq = lax.broadcasted_iota(jnp.int32, (160, 128), 1)
    jk = lax.rem(row_i, 16)
    win = 3 * (row_i // 16 - 1) + jk
    off = SPAN - 1 + jq - win
    seen = jnp.zeros((160, 128), jnp.bool_)
    for t in range(16):
        mine = jnp.where(jq == 0, lay_ref[0, t], jnp.where(jq == 1, lay_ref[1, t], lay_ref[2, t]))
        seen = seen | (off == mine)
    seen = seen & (off >= 0) & (3 * s - (SPAN - 1) + win >= 0)
    mask = jnp.where(seen | (jk >= 3), 0.0, NEG).astype(BF16)
    for h in range(4):
        qst[h, 576:736] = mask
    spread(q_copy)

    idm[...] = jnp.full((8, 256), 5.0, F32)
    idm[:, 0:OWN] = jnp.broadcast_to(ids_ref[...].astype(F32), (8, OWN))
    rwr[...] = jnp.zeros((8, 256), F32)
    rwr[:, 0:OWN] = jnp.broadcast_to(rw_ref[...], (8, OWN))
    rwc[...] = jnp.transpose(jnp.broadcast_to(rwr[0:1], (128, 256)))[0:OWN]
    send_id = pltpu.make_async_remote_copy(
        src_ref=idm, dst_ref=idr, send_sem=s_id, recv_sem=r_id, device_id=(s, 1 - e), device_id_type=MESH
    )
    send_id.start()

    @pl.when(c == ct)
    def _():
        kv[8 + p] = kst[x]
        qraw[lax.rem(p, 4)] = qst[x]

    def kv_wait(slot):
        pltpu.make_async_remote_copy(
            src_ref=kst.at[0], dst_ref=kv.at[slot], send_sem=s_kv.at[0], recv_sem=r_kv.at[slot],
            device_id=at(r, x, 1 - c, e), device_id_type=MESH,
        ).wait_recv()

    def to_core1(slot):
        return pltpu.make_async_remote_copy(
            src_ref=kv.at[slot], dst_ref=kv.at[slot], send_sem=s_f.at[slot], recv_sem=r_kv.at[slot],
            device_id=at(r, x, 1, e), device_id_type=MESH,
        )

    def to_next(slot):
        return pltpu.make_async_remote_copy(
            src_ref=kv.at[slot], dst_ref=kv.at[slot - 8], send_sem=s_row.at[slot - 8], recv_sem=r_kv.at[slot - 8],
            device_id=at(nxt, x, 0, e), device_id_type=MESH,
        )

    def unpack(slot):
        t = kv[slot, 384:576].astype(F32)
        for part, val in ((0, t), (1, pltpu.roll(t, 64, 1))):
            lane = lax.broadcasted_iota(jnp.int32, val.shape, 1)
            block = (lax.broadcasted_iota(jnp.int32, val.shape, 0) + part * OWN) // 128
            mark = jnp.where(lane == 64 + block, 1.0, 0.0)
            kt[slot, part * OWN : part * OWN + OWN] = jnp.where(lane < 64, val, mark).astype(BF16)

    m_sc[...] = jnp.full((2, 8, PAIR), -3e38, F32)
    l_sc[...] = jnp.zeros((2, 8, PAIR), F32)
    acc[...] = jnp.zeros((2, 128, PAIR), F32)
    bias[...] = jnp.full((2, 12, 16, PAIR), NEG, BF16)
    qb[...] = jnp.zeros((2, 256, PAIR), BF16)

    def arrive(i, carry):
        slot = 8 + 4 * c + lax.rem(2 * lax.rem(x, 2) + i, 4)

        @pl.when(slot != 8 + p)
        def _():
            kv_wait(slot)

        @pl.when(slot > 8)
        def _():
            to_next(slot).start()

        @pl.when(c == 0)
        def _():
            to_core1(slot).start()

        unpack(slot)
        return carry

    lax.fori_loop(0, 4, arrive, 0)

    w_out = []
    for d, who in ((0, up), (1, down)):
        quarter = pl.multiple_of((2 * c + d) * 128, 128)
        one = pltpu.make_async_remote_copy(
            src_ref=ow_ref.at[pl.ds(quarter, 128)],
            dst_ref=wb.at[e, pl.ds(quarter, 128)],
            send_sem=s_w.at[d],
            recv_sem=r_w.at[2 * c + d],
            device_id=who,
            device_id_type=MESH,
        )
        one.start()
        w_out.append(one)

    for g in range(4):

        @pl.when(4 * c + g != p)
        def _():
            pltpu.make_async_remote_copy(
                src_ref=qst.at[0], dst_ref=qraw.at[g], send_sem=s_q.at[0], recv_sem=r_q.at[g],
                device_id=at(r, x, 1 - c, e), device_id_type=MESH,
            ).wait_recv()

        odd = g % 2
        for j in range(3):
            cols = slice(odd * TOK + j * 128, odd * TOK + j * 128 + 128)
            qb[g // 2, 0:192, cols] = qraw[g, j * 192 : j * 192 + 192]
            for k in range(10):
                b = qraw[g, 576 + 16 * k : 592 + 16 * k].astype(F32)
                bias[g // 2, k + odd, :, cols] = jnp.broadcast_to(b[:, j : j + 1], (16, 128)).astype(BF16)

    score_buf = (sa, sb)
    prob_buf = (pa, pb)

    def tiles(work):
        chunks = [(pair, slot, diag, n) for pair, slot, diag in work for n in range(PAIR // 256)]
        fades = [None] * len(chunks)

        def scores(i):
            pair, slot, diag, n = chunks[i]
            if n == 0:
                qb[pair, 192:208] = bias[pair, slot - (4 * c + 2 * pair)]
            keys = jnp.concatenate([kv[slot, 0:384], kt[slot]], axis=1)
            score_buf[i % 2][...] = jnp.dot(
                keys, qb[pair, :, n * 256 : n * 256 + 256], preferred_element_type=F32
            )

        def probabilities(i):
            pair, slot, diag, n = chunks[i]
            cols = slice(n * 256, n * 256 + 256)
            parts = []
            for j in range(3):
                sj = score_buf[i % 2][j * 128 : j * 128 + 128]
                if diag:
                    ki = lax.broadcasted_iota(jnp.int32, (128, 256), 0) + j * 128
                    qi = lax.broadcasted_iota(jnp.int32, (128, 256), 1) + n * 256
                    sj = jnp.where(ki <= qi + TOK * (8 + 4 * c + 2 * pair - slot), sj, NEG)
                parts.append(sj)
            top = jnp.max(jnp.maximum(jnp.maximum(parts[0], parts[1]), parts[2]), axis=0, keepdims=True)
            m_old = m_sc[pair, 0:1, cols]
            m_new = jnp.maximum(m_old, top)
            fades[i] = jnp.exp2((m_old - m_new) * COEF)
            m_sc[pair, :, cols] = jnp.broadcast_to(m_new, (8, 256))
            mass = jnp.zeros((8, 256), F32)
            for j in range(3):
                pj = jnp.exp2((parts[j] - m_new) * COEF)
                mass = mass + jnp.sum(pj.reshape(16, 8, 256), axis=0)
                prob_buf[i % 2][j * 128 : j * 128 + 128] = pj.astype(BF16)
            l_sc[pair, :, cols] = l_sc[pair, :, cols] * fades[i] + mass

        def context(i):
            pair, slot, diag, n = chunks[i]
            cols = slice(n * 256, n * 256 + 256)
            vals = jnp.concatenate([kv[slot, 576 + j * 128 : 704 + j * 128] for j in range(3)], axis=1)
            acc[pair, :, cols] = acc[pair, :, cols] * fades[i] + jnp.dot(
                vals, prob_buf[i % 2][...], preferred_element_type=F32
            )

        for t in range(len(chunks) + 2):
            if t < len(chunks):
                scores(t)
            if 0 <= t - 1 < len(chunks):
                probabilities(t - 1)
            if t >= 2:
                context(t - 2)

    def early(i, carry):
        slot = 8 + i
        kv_wait(slot)
        unpack(slot)
        tiles([(0, slot, False), (1, slot, False)])
        return carry

    lax.fori_loop(0, 4 * c, early, 0)

    base = 8 + 4 * c
    tiles(
        [
            (0, base, True),
            (1, base, False),
            (0, base + 1, True),
            (1, base + 1, False),
            (1, base + 2, True),
            (1, base + 3, True),
        ]
    )

    def prev_row(i, carry):
        half = i // 2
        odd = i - 2 * half
        slot = (1 - c) * (7 - 4 * odd - half) + c * (7 - i)
        kv_wait(slot)

        @pl.when((c == 0) & (slot >= 5))
        def _():
            to_core1(slot).start()

        unpack(slot)

        @pl.when(slot >= 4 * c + 3)
        def _():
            tiles([(0, slot, False), (1, slot, False)])

        @pl.when(slot < 4 * c + 3)
        def _():
            tiles([(0, slot, False)])

        return carry

    lax.fori_loop(0, 7 - 4 * c, prev_row, 0)

    head = 4 * e + x

    def ctx_copy(g, de, kind):
        to_e = lax.rem(e + de, 2)
        side = kind * to_e + (1 - kind) * (1 - to_e)
        return pltpu.make_async_remote_copy(
            src_ref=cst.at[g, side], dst_ref=ctx.at[kind, head],
            send_sem=s_c.at[4 * g + 2 * de + kind], recv_sem=r_c.at[8 * kind + head],
            device_id=at(r, 2 * c + g // 2, lax.rem(g, 2), to_e), device_id_type=MESH,
        )

    for g in range(4):
        lanes = slice((g % 2) * TOK, (g % 2) * TOK + TOK)
        total = jnp.sum(l_sc[g // 2, :, lanes], axis=0, keepdims=True)
        res = jnp.transpose(acc[g // 2, :, lanes] / total).astype(BF16)
        cst[g, 0] = res[0:OWN]
        cst[g, 1] = res[OWN:TOK]

        ctx_copy(g, 1, 0).start()

        @pl.when(4 * c + g != p)
        def _():
            ctx_copy(g, 0, 0).start()

        @pl.when(4 * c + g == p)
        def _():
            ctx[0, head] = cst[g, 1 - e]
            ctx[1, head] = cst[g, e]

    for g in range(4):
        ctx_copy(g, 1, 1).start()

        @pl.when(4 * c + g != p)
        def _():
            ctx_copy(g, 0, 1).start()

    def w_copy(quarter):
        start = pl.multiple_of(quarter * 128, 128)
        return pltpu.make_async_remote_copy(
            src_ref=wb.at[1 - e, pl.ds(start, 128)], dst_ref=wb.at[1 - e, pl.ds(start, 128)],
            send_sem=s_w.at[2 + lax.rem(quarter, 2)], recv_sem=r_w.at[quarter],
            device_id=at(r, x, 1 - c, e), device_id_type=MESH,
        )

    for d in range(2):
        w_copy(2 * c + d).wait_recv()
        w_copy(2 * c + d).start()

    send_id.wait_recv()
    upper = (
        lax.broadcasted_iota(jnp.int32, (256, 256), 0) <= lax.broadcasted_iota(jnp.int32, (256, 256), 1)
    ).astype(BF16)
    for n, (src, who) in enumerate(((idr, e), (idm, e), (idm, 1 - e))):
        member = (src[...] == who.astype(F32)).astype(F32)
        member = jnp.concatenate([member, member], axis=0)
        rank = jnp.dot(member.astype(BF16), upper, preferred_element_type=F32)
        rank = jnp.where(member > 0.5, rank - 1.0, -1.0)[0:1]
        slots = lax.broadcasted_iota(jnp.int32, (CAP, 256), 0).astype(F32)
        pm[n] = jnp.where(slots == rank, 1.0, 0.0).astype(BF16)
    nrm[OWN:256] = jnp.zeros((64, D), BF16)

    for one in loads:
        one.wait()
    for d in range(2):
        w_copy(2 * (1 - c) + d).wait_recv()

    def ret_copy(n):
        return pltpu.make_async_remote_copy(
            src_ref=rst.at[n], dst_ref=ret.at[n], send_sem=s_ret.at[n], recv_sem=r_ret.at[n],
            device_id=(s, 1 - e), device_id_type=MESH,
        )

    def expert_pass(kind):
        def ctx_wait(h, carry):
            @pl.when((h != head) | (c != ct))
            def _():
                pltpu.make_async_remote_copy(
                    src_ref=cst.at[0, 0], dst_ref=ctx.at[kind, h], send_sem=s_c.at[0], recv_sem=r_c.at[8 * kind + h],
                    device_id=at(r, x, 1 - c, e), device_id_type=MESH,
                ).wait_recv()

            return carry

        lax.fori_loop(0, 8, ctx_wait, 0)

        def project(n, carry):
            cols = pl.ds(pl.multiple_of(n * WCH, WCH), WCH)
            total = jnp.zeros((OWN, WCH), F32)
            for side in range(2):
                left = jnp.concatenate([ctx[kind, 4 * side + i] for i in range(4)], axis=1)
                total = total + jnp.dot(left, wb[side, :, cols], preferred_element_type=F32)
            att[:, cols] = total
            sq = total * total
            part = sq[:, 0:128]
            for i in range(1, WCH // 128):
                part = part + sq[:, i * 128 : i * 128 + 128]
            return carry + part

        sums = lax.fori_loop(0, NCH, project, jnp.zeros((OWN, 128), F32))
        scale = lax.rsqrt(jnp.sum(sums, axis=1, keepdims=True) * (1.0 / D) + 1e-06)

        def normalize(n, carry):
            cols = pl.ds(pl.multiple_of(n * WCH, WCH), WCH)
            nrm[0:OWN, cols] = (att[:, cols] * scale * gain_ref[:, cols]).astype(BF16)
            rows[:, cols] = jnp.dot(pm[kind], nrm[:, cols], preferred_element_type=F32).astype(BF16)
            return carry

        lax.fori_loop(0, NCH, normalize, 0)

        last = (((1,), (1,)), ((), ()))
        gate = lax.dot_general(rows[...], gwb[...], last, preferred_element_type=F32)
        upp = lax.dot_general(rows[...], uwb[...], last, preferred_element_type=F32)
        hidden = (gate * jax.nn.sigmoid(gate) * upp).astype(BF16)
        for n in range(NCH):
            cols = slice(n * WCH, n * WCH + WCH)
            res = jnp.dot(hidden, dwb[:, cols], preferred_element_type=F32).astype(BF16)
            if kind == 0:
                rst[n] = res
                ret_copy(n).start()
            else:
                own_res[n] = res

    expert_pass(0)
    expert_pass(1)

    for n in range(NCH):
        cols = slice(n * WCH, n * WCH + WCH)
        got = lax.dot_general(pm[1], own_res[n], (((0,), (0,)), ((), ())), preferred_element_type=F32)
        ret_copy(n).wait_recv()
        got = got + lax.dot_general(pm[2], ret[n], (((0,), (0,)), ((), ())), preferred_element_type=F32)
        out_ref[:, cols] = (att[:, cols] + rwc[:, 0:1] * got[0:OWN]).astype(BF16)

    for n in range(NCH):
        ret_copy(n).wait_send()
    for d in (1, 2, 3):
        kv_copy(d).wait_send()
        q_copy(d).wait_send()

    @pl.when(c != ct)
    def _():
        kv_copy(0).wait_send()
        q_copy(0).wait_send()

    def sent(i, carry):
        slot = 8 + 4 * c + i

        @pl.when(slot > 8)
        def _():
            to_next(slot).wait_send()

        @pl.when(c == 0)
        def _():
            to_core1(slot).wait_send()

        return carry

    lax.fori_loop(0, 4, sent, 0)

    def sent_prev(i, carry):
        to_core1(5 + i).wait_send()
        return carry

    lax.fori_loop(0, 3 - 3 * c, sent_prev, 0)

    def sent_ctx(g, carry):
        for kind in range(2):
            ctx_copy(g, 1, kind).wait_send()

        @pl.when(4 * c + g != p)
        def _():
            for kind in range(2):
                ctx_copy(g, 0, kind).wait_send()

        return carry

    lax.fori_loop(0, 4, sent_ctx, 0)
    for one in w_out:
        one.wait_send()
    for d in range(2):
        w_copy(2 * c + d).wait_send()
    send_id.wait_send()


def shards(
    queries, key_heads, value_heads, block_layout, out_weight, norm_gain, expert_ids, route_weight,
    gate_weight, up_weight, down_weight,
):
    vm = pl.BlockSpec(memory_space=pltpu.VMEM)
    anyspace = pl.BlockSpec(memory_space=pl.ANY)
    dma = pltpu.SemaphoreType.DMA
    return pl.pallas_call(
        kernel,
        out_shape=jax.ShapeDtypeStruct((OWN, D), BF16),
        in_specs=[anyspace] * 3 + [pl.BlockSpec(memory_space=pltpu.SMEM), vm, vm, vm] + [anyspace] * 4,
        out_specs=vm,
        scratch_shapes=[
            pltpu.VMEM((TOK, 768), BF16),
            pltpu.VMEM((TOK, 768), BF16),
            pltpu.VMEM((TOK, 512), BF16),
            pltpu.VMEM((4, KVR, 128), BF16),
            pltpu.VMEM((4, QR, 128), BF16),
            pltpu.VMEM((16, KVR, 128), BF16),
            pltpu.VMEM((16, TOK, 128), BF16),
            pltpu.VMEM((4, QR, 128), BF16),
            pltpu.VMEM((2, 256, PAIR), BF16),
            pltpu.VMEM((2, 12, 16, PAIR), BF16),
            pltpu.VMEM((2, 8, PAIR), F32),
            pltpu.VMEM((2, 8, PAIR), F32),
            pltpu.VMEM((2, 128, PAIR), F32),
            pltpu.VMEM((TOK, 256), F32),
            pltpu.VMEM((TOK, 256), F32),
            pltpu.VMEM((TOK, 256), BF16),
            pltpu.VMEM((TOK, 256), BF16),
            pltpu.VMEM((4, 2, OWN, 128), BF16),
            pltpu.VMEM((2, 8, OWN, 128), BF16),
            pltpu.VMEM((2, 512, D), BF16),
            pltpu.VMEM((FF, D), BF16),
            pltpu.VMEM((FF, D), BF16),
            pltpu.VMEM((FF, D), BF16),
            pltpu.VMEM((8, 256), F32),
            pltpu.VMEM((8, 256), F32),
            pltpu.VMEM((8, 256), F32),
            pltpu.VMEM((OWN, 128), F32),
            pltpu.VMEM((OWN, D), F32),
            pltpu.VMEM((256, D), BF16),
            pltpu.VMEM((CAP, D), BF16),
            pltpu.VMEM((NCH, CAP, WCH), BF16),
            pltpu.VMEM((NCH, CAP, WCH), BF16),
            pltpu.VMEM((NCH, CAP, WCH), BF16),
            pltpu.VMEM((3, CAP, 256), BF16),
            dma((7,)),
            dma((4,)), dma((16,)),
            dma((4,)), dma((4,)),
            dma((16,)), dma((8,)),
            dma((16,)), dma((16,)),
            dma((4,)), dma((4,)),
            dma, dma,
            dma((NCH,)), dma((NCH,)),
        ],
        compiler_params=pltpu.CompilerParams(
            collective_id=0, has_side_effects=True, vmem_limit_bytes=60 * 1024 * 1024
        ),
        name="layer",
    )(
        queries, key_heads, value_heads, block_layout, norm_gain.reshape(1, D), expert_ids.reshape(1, OWN),
        route_weight.reshape(1, OWN), out_weight, gate_weight[0].T, up_weight[0].T, down_weight[0],
    )


def solution(mesh):
    in_specs = (
        P("seq", "exp"),
        P("seq", "exp"),
        P("seq", "exp"),
        P("seq", None),
        P("exp", None),
        P(),
        P(("seq", "exp"), None),
        P(("seq", "exp"), None),
        P("exp", None, None),
        P("exp", None, None),
        P("exp", None, None),
    )
    out_specs = P(("seq", "exp"), None)
    return jax.shard_map(shards, mesh=mesh, in_specs=in_specs, out_specs=out_specs, check_vma=False)
```
